8 devices in a mesh: dp: 8 (over z, y, x, core).
Axes of the slice: x: 2, y: 2, z: 1, core: 2. Of those that a mesh axis runs over, the one named last changes fastest.
Arguments:
- x_saved: bfloat16 [8, 1024, 960], P('dp')
- grad_out: bfloat16 [8, 1024, 960], P('dp')
- positions: int32 [8, 1024], P('dp')
- attn_gain: bfloat16 [960], replicated
- w_query: bfloat16 [960, 15, 64], replicated
- w_key: bfloat16 [960, 5, 64], replicated
- w_value: bfloat16 [960, 5, 64], replicated
- w_out: bfloat16 [15, 64, 960], replicated
- mlp_gain: bfloat16 [960], replicated
- w_gate: bfloat16 [960, 2560], replicated
- w_up: bfloat16 [960, 2560], replicated
- w_down: bfloat16 [2560, 960], replicated
- master_flat: float32 [9832320], P('dp')
- adam_mean: float32 [9832320], P('dp')
- adam_var: float32 [9832320], P('dp')
Outputs:
- output 1: bfloat16 [8, 1024, 960], P('dp')
- output 2: bfloat16 [960], replicated
- output 3: bfloat16 [960, 15, 64], replicated
- output 4: bfloat16 [960, 5, 64], replicated
- output 5: bfloat16 [960, 5, 64], replicated
- output 6: bfloat16 [15, 64, 960], replicated
- output 7: bfloat16 [960], replicated
- output 8: bfloat16 [960, 2560], replicated
- output 9: bfloat16 [960, 2560], replicated
- output 10: bfloat16 [2560, 960], replicated
- output 11: float32 [9832320], P('dp')
- output 12: float32 [9832320], P('dp')
- output 13: float32 [9832320], P('dp')
- output 14: float32 [], replicated
All inputs are finite; a program needn't handle non-finite values.
Results may differ from the reference program's by a relative error of at most 0.0122752.
Values are sent between devices in bfloat16 or wider.
A program may use at most 1 GiB of HBM per device.

```python
import math
import jax
import jax.numpy as jnp
from jax import lax

MODEL_DIM = 960
NUM_HEADS = 15
KV_HEADS = 5
HEAD_DIM = 64
FFN_DIM = 2560
SEQ_LEN = 1024
SEQS_DEV = 1
DP_SIZE = 8
STEP_COUNT = 100
TOTAL_SEQS = SEQS_DEV * DP_SIZE
NPARAM = MODEL_DIM * (2 + 2 * HEAD_DIM * (NUM_HEADS + KV_HEADS) + 3 * FFN_DIM)
NORM_EPS = 1e-5
ROPE_BASE = 10000.0
LEARN_RATE = 2e-3
BETA_ONE = 0.9
BETA_TWO = 0.95
ADAM_EPS = 1e-8
WEIGHT_DECAY = 0.1


def param_shapes():
    return [(MODEL_DIM,), (MODEL_DIM, NUM_HEADS, HEAD_DIM), (MODEL_DIM, KV_HEADS, HEAD_DIM),
            (MODEL_DIM, KV_HEADS, HEAD_DIM), (NUM_HEADS, HEAD_DIM, MODEL_DIM), (MODEL_DIM,),
            (MODEL_DIM, FFN_DIM), (MODEL_DIM, FFN_DIM), (FFN_DIM, MODEL_DIM)]


def draw_params(key):
    key_list = jax.random.split(key, 9)
    fan_ins = [0, MODEL_DIM, MODEL_DIM, MODEL_DIM, NUM_HEADS * HEAD_DIM, 0, MODEL_DIM, MODEL_DIM, FFN_DIM]
    drawn_list = []
    for number, piece_shape in enumerate(param_shapes()):
        noise_arr = jax.random.normal(key_list[number], piece_shape, jnp.float32)
        if fan_ins[number] == 0:
            drawn_list.append(1.0 + 0.2 * noise_arr)
        else:
            drawn_list.append(noise_arr * fan_ins[number] ** -0.5)
    return drawn_list


def setup_inputs(seed: int = 0) -> dict:
    key_list = jax.random.split(jax.random.key(seed), 8)
    act_shape = (TOTAL_SEQS, SEQ_LEN, MODEL_DIM)
    x_saved = jax.random.normal(key_list[0], act_shape, jnp.float32).astype(jnp.bfloat16)
    grad_out = jax.random.normal(key_list[1], act_shape, jnp.float32).astype(jnp.bfloat16)
    pos_gaps = jax.random.randint(key_list[2], (TOTAL_SEQS, SEQ_LEN), 1, 4)
    positions = (jnp.cumsum(pos_gaps, axis=1) - 1).astype(jnp.int32)
    weights = [w_piece.astype(jnp.bfloat16) for w_piece in draw_params(key_list[3])]
    master_flat = jnp.concatenate([w_piece.reshape(-1) for w_piece in draw_params(key_list[4])])
    state_scale = NPARAM ** -0.5
    adam_mean = 0.1 * state_scale * jax.random.normal(key_list[5], (NPARAM,), jnp.float32)
    var_root = 0.3 * state_scale * jax.random.uniform(key_list[6], (NPARAM,), jnp.float32, 0.5, 1.5)
    adam_var = var_root * var_root
    return {'x_saved': x_saved, 'grad_out': grad_out, 'positions': positions,
            'attn_gain': weights[0], 'w_query': weights[1], 'w_key': weights[2], 'w_value': weights[3],
            'w_out': weights[4], 'mlp_gain': weights[5], 'w_gate': weights[6], 'w_up': weights[7],
            'w_down': weights[8], 'master_flat': master_flat, 'adam_mean': adam_mean, 'adam_var': adam_var}


def rms_scale(values, gain):
    wide = values.astype(jnp.float32)
    inv_rms = lax.rsqrt(jnp.mean(wide * wide, axis=-1, keepdims=True) + NORM_EPS)
    return (wide * inv_rms * gain.astype(jnp.float32)).astype(jnp.bfloat16)


def rope_tables(positions, head_dim):
    half_dim = head_dim // 2
    inv_freq = ROPE_BASE ** (-2.0 * jnp.arange(half_dim, dtype=jnp.float32) / head_dim)
    angles = positions.astype(jnp.float32)[:, :, None] * inv_freq
    cos_full = jnp.concatenate([jnp.cos(angles), jnp.cos(angles)], axis=-1)[:, :, None, :]
    sin_full = jnp.concatenate([jnp.sin(angles), jnp.sin(angles)], axis=-1)[:, :, None, :]
    return cos_full, sin_full


def rope_apply(values, cos_full, sin_full):
    half_dim = values.shape[-1] // 2
    rotated = jnp.concatenate([-values[..., half_dim:], values[..., :half_dim]], axis=-1)
    return values * cos_full + rotated * sin_full


def layer_forward(w_list, x_val, positions):
    attn_gain, w_query, w_key, w_value, w_out, mlp_gain, w_gate, w_up, w_down = w_list
    num_seqs, seq_len, model_dim = x_val.shape
    num_heads, head_dim = w_query.shape[1], w_query.shape[2]
    kv_heads = w_key.shape[1]
    group_size = num_heads // kv_heads
    n_tok = num_seqs * seq_len
    x_flat = x_val.reshape(n_tok, model_dim)
    normed = rms_scale(x_flat, attn_gain)
    q_pre = jnp.dot(normed, w_query.reshape(model_dim, num_heads * head_dim), preferred_element_type=jnp.float32)
    k_pre = jnp.dot(normed, w_key.reshape(model_dim, kv_heads * head_dim), preferred_element_type=jnp.float32)
    v_pre = jnp.dot(normed, w_value.reshape(model_dim, kv_heads * head_dim), preferred_element_type=jnp.float32)
    v_heads = v_pre.astype(jnp.bfloat16).reshape(num_seqs, seq_len, kv_heads, head_dim)
    cos_full, sin_full = rope_tables(positions, head_dim)
    q_rot = rope_apply(q_pre.reshape(num_seqs, seq_len, num_heads, head_dim), cos_full, sin_full).astype(jnp.bfloat16)
    q_rot = q_rot.reshape(num_seqs, seq_len, kv_heads, group_size, head_dim)
    k_rot = rope_apply(k_pre.reshape(num_seqs, seq_len, kv_heads, head_dim), cos_full, sin_full).astype(jnp.bfloat16)
    scores = jnp.einsum('bqkgd,bskd->bkgqs', q_rot.astype(jnp.float32), k_rot.astype(jnp.float32)) * head_dim ** -0.5
    causal = jnp.arange(seq_len)[:, None] >= jnp.arange(seq_len)[None, :]
    attn_probs = jax.nn.softmax(jnp.where(causal, scores, -1e30), axis=-1).astype(jnp.bfloat16)
    context = jnp.einsum('bkgqs,bskd->bqkgd', attn_probs.astype(jnp.float32), v_heads.astype(jnp.float32)).astype(jnp.bfloat16)
    attn_out = jnp.dot(context.reshape(n_tok, num_heads * head_dim), w_out.reshape(num_heads * head_dim, model_dim), preferred_element_type=jnp.float32)
    hidden = (x_flat.astype(jnp.float32) + attn_out).astype(jnp.bfloat16)
    normed_mlp = rms_scale(hidden, mlp_gain)
    gate_pre = jnp.dot(normed_mlp, w_gate, preferred_element_type=jnp.float32)
    up_pre = jnp.dot(normed_mlp, w_up, preferred_element_type=jnp.float32)
    gated_act = (jax.nn.silu(gate_pre) * up_pre).astype(jnp.bfloat16)
    down_out = jnp.dot(gated_act, w_down, preferred_element_type=jnp.float32)
    return (hidden.astype(jnp.float32) + down_out).astype(jnp.bfloat16).reshape(num_seqs, seq_len, model_dim)


def split_flat(flat_vec):
    pieces = []
    offset = 0
    for piece_shape in param_shapes():
        piece_size = math.prod(piece_shape)
        pieces.append(flat_vec[offset:offset + piece_size].reshape(piece_shape))
        offset += piece_size
    return pieces


def reference(x_saved, grad_out, positions, attn_gain, w_query, w_key, w_value, w_out, mlp_gain, w_gate, w_up, w_down, master_flat, adam_mean, adam_var):
    w_list = (attn_gain, w_query, w_key, w_value, w_out, mlp_gain, w_gate, w_up, w_down)

    def device_grads(grad_acc, group_in):
        x_group, dy_group, pos_group = group_in
        layer_out, pullback = jax.vjp(lambda x_val, w_vals: layer_forward(w_vals, x_val, pos_group), x_group, w_list)
        grad_x, grad_w = pullback(dy_group)
        flat_grad = jnp.concatenate([w_grad.astype(jnp.bfloat16).reshape(-1).astype(jnp.float32) for w_grad in grad_w])
        return grad_acc + flat_grad, grad_x.astype(jnp.bfloat16)

    group_shape = (DP_SIZE, SEQS_DEV, SEQ_LEN, MODEL_DIM)
    grad_sum, grad_x = lax.scan(device_grads, jnp.zeros((NPARAM,), jnp.float32),
                                (x_saved.reshape(group_shape), grad_out.reshape(group_shape),
                                 positions.reshape(DP_SIZE, SEQS_DEV, SEQ_LEN)))
    grad_mean = grad_sum / DP_SIZE
    grad_norm = jnp.sqrt(jnp.sum(grad_mean * grad_mean))
    clip_scale = jnp.minimum(1.0, 1.0 / (grad_norm + 1e-6))
    clipped = grad_mean * clip_scale
    new_mean = BETA_ONE * adam_mean + (1.0 - BETA_ONE) * clipped
    new_var = BETA_TWO * adam_var + (1.0 - BETA_TWO) * clipped * clipped
    mean_hat = new_mean / (1.0 - BETA_ONE ** STEP_COUNT)
    var_hat = new_var / (1.0 - BETA_TWO ** STEP_COUNT)
    gain_two = MODEL_DIM + 2 * MODEL_DIM * HEAD_DIM * (NUM_HEADS + KV_HEADS)
    flat_index = jnp.arange(NPARAM)
    is_gain = (flat_index < MODEL_DIM) | ((flat_index >= gain_two) & (flat_index < gain_two + MODEL_DIM))
    decays = jnp.where(is_gain, 0.0, WEIGHT_DECAY)
    new_master = master_flat - LEARN_RATE * (mean_hat / (jnp.sqrt(var_hat) + ADAM_EPS) + decays * master_flat)
    new_weights = split_flat(new_master.astype(jnp.bfloat16))
    return (grad_x.reshape(TOTAL_SEQS, SEQ_LEN, MODEL_DIM), new_weights[0], new_weights[1], new_weights[2],
            new_weights[3], new_weights[4], new_weights[5], new_weights[6], new_weights[7], new_weights[8],
            new_master, new_mean, new_var, grad_norm)
```

```python
import functools
import jax
import jax.numpy as jnp
from jax import lax
from jax.experimental import pallas as pl
from jax.experimental.pallas import tpu as pltpu
from jax.sharding import PartitionSpec as P

N0 = 0
F1_0 = 1.0
N1 = 1
N2 = 2
N3 = 3
N4 = 4
N5 = 5
N6 = 6
N7 = 7
N8 = 8
N9 = 9
N10 = 10
N15 = 15
N16 = 16
N20 = 20
N24 = 24
N32 = 32
N40 = 40
N48 = 48
N64 = 64
N112 = 112
N128 = 128
N240 = 240
N320 = 320
N480 = 480
N960 = 960
N1024 = 1024
N1280 = 1280
N2560 = 2560

NORM_EPS = 1e-5
ROPE_BASE = 10000.0
LEARN_RATE = 2e-3
BETA_ONE = 0.9
BETA_TWO = 0.95
ADAM_EPS = 1e-8
WEIGHT_DECAY = 0.1
STEP_COUNT = 100

SEQ, DIM, HEADS, KVH, HD, FFN = N1024, N960, N15, N5, N64, N2560
GROUP = HEADS // KVH
QB = 256
QF = 512
MESH = pl.DeviceIdType.MESH
F32, BF16 = jnp.float32, jnp.bfloat16


def dotf(a, b, ca, cb):
    return lax.dot_general(a, b, (((ca,), (cb,)), ((), ())), preferred_element_type=F32)


def rope(v, cos, sin):
    a, b = v[:HD // N2], v[HD // N2:]
    return jnp.concatenate([a * cos - b * sin, b * cos + a * sin], axis=N0)


def rope_t(g, cos, sin):
    a, b = g[:HD // N2], g[HD // N2:]
    return jnp.concatenate([a * cos + b * sin, b * cos - a * sin], axis=N0)


def masked_scores(k, q, j, qb):
    s = dotf(k, q, N1, N0)
    rows = lax.broadcasted_iota(jnp.int32, (qb, qb), N0)
    cols = lax.broadcasted_iota(jnp.int32, (qb, qb), N1)
    diag = jnp.where(rows <= cols, s[j * qb:], -1e30)
    return diag if j == N0 else jnp.concatenate([s[:j * qb], diag], axis=N0)


def attn_fwd_kernel(q_ref, k_ref, v_ref, cos_ref, sin_ref, ctx_ref, lse_ref, qr_ref, kr_ref):
    cos, sin = cos_ref[...], sin_ref[...]
    q = rope(q_ref[...], cos, sin).astype(BF16)
    k = rope(k_ref[...], cos, sin).astype(BF16)
    q = q * jnp.asarray(HD ** -0.5, BF16)
    qr_ref[...] = q
    kr_ref[...] = k
    kt = k.T
    v = v_ref[...]
    for j in range(SEQ // QF):
        hi = (j + N1) * QF
        cs = slice(j * QF, hi)
        s = masked_scores(kt[:hi], q[:, cs], j, QF)
        m = jnp.max(s, axis=N0, keepdims=True)
        e = jnp.exp(s - m)
        l = jnp.sum(e, axis=N0, keepdims=True)
        p = (e * (F1_0 / l)).astype(BF16)
        ctx_ref[:, cs] = dotf(v[:, :hi], p, N1, N0).astype(BF16)
        lse_ref[N0, :, cs] = m + jnp.log(l)


def attn_bwd_kernel(q_ref, k_ref, v_ref, ctx_ref, dctx_ref, lse_ref, cos_ref, sin_ref,
                    dq_ref, dk_ref, dv_ref):
    first = pl.program_id(N0) % GROUP == N0

    @pl.when(first)
    def _():
        dk_ref[...] = jnp.zeros_like(dk_ref)
        dv_ref[...] = jnp.zeros_like(dv_ref)

    k, v = k_ref[...], v_ref[...]
    kt, vt = k.T, v.T
    k_scaled = k * jnp.asarray(HD ** -0.5, BF16)
    delta = jnp.sum(ctx_ref[...].astype(F32) * dctx_ref[...].astype(F32), axis=N0, keepdims=True)
    for j in range(SEQ // QB):
        hi = (j + N1) * QB
        cs = slice(j * QB, hi)
        q, do = q_ref[:, cs], dctx_ref[:, cs]
        p = jnp.exp(masked_scores(kt[:hi], q, j, QB) - lse_ref[N0, :, cs])
        dp = dotf(vt[:hi], do, N1, N0)
        ds = (p * (dp - delta[:, cs])).astype(BF16)
        dv_ref[:, :hi] += dotf(do, p.astype(BF16), N1, N1)
        dk_ref[:, :hi] += dotf(q, ds, N1, N1)
        dq = dotf(k_scaled[:, :hi], ds, N1, N0)
        dq_ref[:, cs] = rope_t(dq, cos_ref[:, cs], sin_ref[:, cs]).astype(BF16)


def head_spec():
    return pl.BlockSpec((HD, SEQ), lambda h: (h, N0))


def group_spec():
    return pl.BlockSpec((HD, SEQ), lambda h: (h // GROUP, N0))


def lse_spec():
    return pl.BlockSpec((N1, N1, SEQ), lambda h: (h, N0, N0))


def table_spec():
    return pl.BlockSpec((HD // N2, SEQ), lambda h: (N0, N0))


def attn_fwd(q, k, v, cos, sin):
    return pl.pallas_call(
        attn_fwd_kernel, grid=(HEADS,),
        in_specs=[head_spec(), group_spec(), group_spec(), table_spec(), table_spec()],
        out_specs=[head_spec(), lse_spec(), head_spec(), group_spec()],
        out_shape=[jax.ShapeDtypeStruct((DIM, SEQ), BF16), jax.ShapeDtypeStruct((HEADS, N1, SEQ), F32),
                   jax.ShapeDtypeStruct((DIM, SEQ), BF16), jax.ShapeDtypeStruct((KVH * HD, SEQ), BF16)],
        compiler_params=pltpu.CompilerParams(vmem_limit_bytes=N40 << N20),
        cost_estimate=pl.CostEstimate(flops=N3 * N10 ** N9, bytes_accessed=N10 ** N7, transcendentals=N10 ** N7),
        name="attn_fwd")(q, k, v, cos, sin)


def attn_bwd(q, k, v, ctx, dctx, lse, cos, sin):
    return pl.pallas_call(
        attn_bwd_kernel, grid=(HEADS,),
        in_specs=[head_spec(), group_spec(), group_spec(), head_spec(), head_spec(), lse_spec(),
                  table_spec(), table_spec()],
        out_specs=[head_spec(), group_spec(), group_spec()],
        out_shape=[jax.ShapeDtypeStruct((DIM, SEQ), BF16), jax.ShapeDtypeStruct((KVH * HD, SEQ), F32),
                   jax.ShapeDtypeStruct((KVH * HD, SEQ), F32)],
        compiler_params=pltpu.CompilerParams(vmem_limit_bytes=N40 << N20),
        cost_estimate=pl.CostEstimate(flops=N8 * N10 ** N9, bytes_accessed=N10 ** N7, transcendentals=N10 ** N7),
        name="attn_bwd")(q, k, v, ctx, dctx, lse, cos, sin)


FT = 256


def mlp_mid_kernel(wg_ref, wu_ref, wd_ref, b_ref, dy_ref, gated_ref, dgate_ref, dup_ref, bt_ref, dyt_ref):
    @pl.when(pl.program_id(N0) == N0)
    def _():
        bt_ref[...] = b_ref[...].T
        dyt_ref[...] = dy_ref[...].T

    gate = dotf(bt_ref[...], wg_ref[...], N1, N0)
    up = dotf(bt_ref[...], wu_ref[...], N1, N0)
    d_gated = dotf(dyt_ref[...], wd_ref[...], N1, N0)
    sig = jax.nn.sigmoid(gate)
    act = gate * sig
    gated_ref[...] = (act * up).astype(BF16)
    dup_ref[...] = (d_gated * act).astype(BF16)
    dgate_ref[...] = (d_gated * up * sig * (F1_0 + gate * (F1_0 - sig))).astype(BF16)


def mlp_mid(w_gate, w_up, wd, b, dy):
    w_spec = pl.BlockSpec((DIM, FT), lambda i: (N0, i))
    act_spec = pl.BlockSpec((DIM, SEQ), lambda i: (N0, N0))
    out_spec = pl.BlockSpec((SEQ, FT), lambda i: (N0, i))
    return pl.pallas_call(
        mlp_mid_kernel, grid=(FFN // FT,),
        in_specs=[w_spec] * N3 + [act_spec] * N2, out_specs=[out_spec] * N3,
        out_shape=[jax.ShapeDtypeStruct((SEQ, FFN), BF16)] * N3,
        scratch_shapes=[pltpu.VMEM((SEQ, DIM), BF16)] * N2,
        compiler_params=pltpu.CompilerParams(vmem_limit_bytes=N48 << N20),
        cost_estimate=pl.CostEstimate(flops=N15 * N10 ** N9, bytes_accessed=34 * N10 ** N6, transcendentals=N10 ** N7),
        name="mlp_mid")(w_gate, w_up, wd, b, dy)


HR, HC = N480, N1280


def mlp_grads_kernel(sel_ref, b_ref, dy_ref, dgate_ref, dup_ref, gated_ref, out_ref):
    s = pl.program_id(N0)

    @pl.when(s == N0)
    def _():
        out_ref[N0, N0] = dotf(b_ref[...], dgate_ref[...], N1, N0).astype(BF16)

    @pl.when(s == N1)
    def _():
        out_ref[N0, N0] = dotf(b_ref[...], dup_ref[...], N1, N0).astype(BF16)

    @pl.when(s == N2)
    def _():
        out_ref[N0, N0] = dotf(dy_ref[...], gated_ref[...], N1, N0).astype(BF16)


def mlp_grads(sel, b, dy, d_gate, d_up, gated):
    def on(s, h, want):
        return jnp.where(s < want, N0, jnp.where(s == want, h, N1))
    grid_spec = pltpu.PrefetchScalarGridSpec(
        num_scalar_prefetch=N1, grid=(N3, N2),
        in_specs=[pl.BlockSpec((HR, SEQ), lambda s, h, sel: (sel[N0], N0)),
                  pl.BlockSpec((HR, SEQ), lambda s, h, sel: (on(s, h, N2), N0)),
                  pl.BlockSpec((SEQ, HC), lambda s, h, sel: (N0, on(s, h, N0))),
                  pl.BlockSpec((SEQ, HC), lambda s, h, sel: (N0, on(s, h, N1))),
                  pl.BlockSpec((SEQ, HC), lambda s, h, sel: (N0, sel[N0]))],
        out_specs=pl.BlockSpec((N1, N1, HR, HC), lambda s, h, sel: (s, h, N0, N0)))
    return pl.pallas_call(
        mlp_grads_kernel, grid_spec=grid_spec,
        out_shape=jax.ShapeDtypeStruct((N3, N2, HR, HC), BF16),
        compiler_params=pltpu.CompilerParams(vmem_limit_bytes=N48 << N20),
        cost_estimate=pl.CostEstimate(flops=75 * N10 ** N8, bytes_accessed=25 * N10 ** N6, transcendentals=N0),
        name="mlp_grads")(sel, b, dy, d_gate, d_up, gated)


def qkv_grads_kernel(a_ref, dq_ref, dk_ref, dv_ref, gq_ref, gk_ref, gv_ref):
    a = a_ref[...]
    gk_ref[...] = dotf(a, dk_ref[...], N1, N1).astype(BF16)
    gv_ref[...] = dotf(a, dv_ref[...], N1, N1).astype(BF16)
    gq_ref[...] = dotf(a, dq_ref[...], N1, N1).astype(BF16)


def qkv_grads(a, dq, dk, dv):
    rows = DIM // N2
    kv = KVH * HD
    return pl.pallas_call(
        qkv_grads_kernel, grid=(N2,),
        in_specs=[pl.BlockSpec((rows, SEQ), lambda i: (i, N0))] + [pl.BlockSpec((n, SEQ), lambda i: (N0, N0)) for n in (DIM, kv, kv)],
        out_specs=[pl.BlockSpec((rows, n), lambda i: (i, N0)) for n in (DIM, kv, kv)],
        out_shape=[jax.ShapeDtypeStruct((DIM, n), BF16) for n in (DIM, kv, kv)],
        compiler_params=pltpu.CompilerParams(vmem_limit_bytes=N48 << N20),
        cost_estimate=pl.CostEstimate(flops=N3 * N10 ** N9, bytes_accessed=N10 ** N7, transcendentals=N0),
        name="qkv_grads")(a, dq, dk, dv)


def hop(v, step, idle=-N1):
    return lax.ppermute(v.astype(BF16), "dp", [(i, i ^ step) for i in range(N8) if i // N2 != idle])


def half_of(own, pair, mask, half):
    shard = jnp.bitwise_xor(lax.axis_index("dp") // N2, mask) - N1
    at = (shard, half, N0, N0)
    take = [lax.dynamic_slice(v, at, (N1, N1, HR, HC)).reshape(HR, HC).astype(F32) for v in (own, pair)]
    return take[N0] + take[N1]


def rms_parts(v):
    inv = lax.rsqrt(jnp.mean(v * v, axis=N0, keepdims=True) + NORM_EPS)
    return inv, v * inv


def rms_back(d_normed, gain, inv, hat):
    d_hat = d_normed * gain
    return inv * (d_hat - hat * jnp.mean(d_hat * hat, axis=N0, keepdims=True))


def local_grads(x, dy, pos, attn_gain, wq, wk, wv, wo, mlp_gain, w_gate, w_up, wd):
    x_wide = x.astype(F32)
    inv_one, x_hat = rms_parts(x_wide)
    gain_one = attn_gain.astype(F32)[:, None]
    a = (x_hat * gain_one).astype(BF16)
    inv_freq = ROPE_BASE ** (-2.0 * jnp.arange(HD // N2, dtype=F32) / HD)
    angles = inv_freq[:, None] * pos.astype(F32)[None, :]
    cos, sin = jnp.cos(angles), jnp.sin(angles)
    q_pre = dotf(wq, a, N1, N0)
    k_pre = dotf(wk, a, N1, N0)
    v = dotf(wv, a, N1, N0).astype(BF16)
    ctx, lse, q, k = attn_fwd(q_pre, k_pre, v, cos, sin)
    hidden = (x_wide + dotf(wo, ctx, N0, N0)).astype(BF16)
    inv_two, h_hat = rms_parts(hidden.astype(F32))
    gain_two = mlp_gain.astype(F32)[:, None]
    b = (h_hat * gain_two).astype(BF16)
    gated, d_gate, d_up = mlp_mid(w_gate, w_up, wd, b, dy)
    core = lax.axis_index("dp") % N2
    send = mlp_grads((N1 - core)[None], b, dy, d_gate, d_up, gated)
    pair = lax.ppermute(send, "dp", [(i, i ^ N1) for i in range(N8)])
    own = mlp_grads(core[None], b, dy, d_gate, d_up, gated)
    d_gate, d_up, own, _ = lax.optimization_barrier((d_gate, d_up, own, send))
    d_b = dotf(w_gate, d_gate, N1, N1) + dotf(w_up, d_up, N1, N1)
    g_mlp_gain = jnp.sum(d_b * h_hat, axis=N1)
    d_hidden = rms_back(d_b, gain_two, inv_two, h_hat) + dy.astype(F32)
    d_hid = d_hidden.astype(BF16)
    g_out = dotf(ctx, d_hid, N1, N1).astype(BF16)
    d_ctx = dotf(wo, d_hid, N1, N0).astype(BF16)
    to_x = jnp.stack([half_of(own, pair, mask, N0) for mask in (N3, N1)]).astype(BF16)
    to_y = jnp.stack([half_of(own, pair, mask, N1) for mask in (N3, N2)]).astype(BF16)
    d_ctx, to_x, to_y = lax.optimization_barrier((d_ctx, to_x, to_y))
    from_x, from_y = hop(to_x, N2), hop(to_y, N4)
    dq, dk_rot, dv_f = attn_bwd(q, k, v, ctx, d_ctx, lse, cos, sin)
    dk = rope_t_all(dk_rot, cos, sin).astype(BF16)
    dv = dv_f.astype(BF16)
    g_query, g_key, g_value = qkv_grads(a, dq, dk, dv)
    g_query, from_x, from_y = lax.optimization_barrier((g_query, from_x, from_y))
    x3 = hop(half_of(own, pair, N1, N1) + from_y[N0].astype(F32), N2, N1)
    y3 = hop(half_of(own, pair, N2, N0) + from_x[N0].astype(F32), N4, N2)
    mlp_parts = own.reshape(N3, DIM, HC), pair.reshape(N3, DIM, HC), (from_x, x3, y3, from_y)
    d_a = dotf(wq, dq, N0, N0) + dotf(wk, dk, N0, N0) + dotf(wv, dv, N0, N0)
    g_attn_gain = jnp.sum(d_a * x_hat, axis=N1)
    d_x = (rms_back(d_a, gain_one, inv_one, x_hat) + d_hidden).astype(BF16)
    return d_x, (g_query, g_key, g_value, g_out), mlp_parts, (g_attn_gain.astype(BF16), g_mlp_gain.astype(BF16))


def rope_t_all(g, cos, sin):
    r = g.reshape(KVH, HD, SEQ)
    a, b = r[:, :HD // N2], r[:, HD // N2:]
    return jnp.concatenate([a * cos + b * sin, b * cos - a * sin], axis=N1).reshape(KVH * HD, SEQ)


FLAT = 9600
LOCAL = 9608
SEGS = {N0: ("A", "B"), N1: ("G",), N2: ("U",), N3: ("D",)}
SHAPE = {"A": (N960, N960), "B": (N960, N320), "G": (N480, N2560), "U": (N480, N2560), "D": (N1280, N960)}
FINAL = {"A": "A", "B": "B", "G": "G", "U": "G", "D": "D"}
SEG_ID = {"A": N0, "B": N1, "G": N2, "U": N3, "D": N4}
RB = N16
CH = 96


def place():
    me = lax.axis_index("dp")
    core = lax.rem(me, N2)
    chip = lax.div(me, N2)
    return me, core, chip


def peer(me, mask):
    out = me
    for bit in (N1, N2, N4):
        if mask & bit:
            out = out + bit - N2 * bit * lax.rem(lax.div(me, bit), N2)
    return out


def greet(me):
    barrier = pltpu.get_barrier_semaphore()
    for mask in range(N1, N8):
        pl.semaphore_signal(barrier, inc=N1, device_id=(peer(me, mask),), device_id_type=MESH)
    pl.semaphore_wait(barrier, N7)


def remote(src, dst, send, recv, to):
    return pltpu.make_async_remote_copy(src_ref=src, dst_ref=dst, send_sem=send, recv_sem=recv,
                                        device_id=(to,), device_id_type=MESH)


def half_rows(seg, half):
    rows = SHAPE[seg][N0] // N2
    return pl.ds(half * rows, rows)


def lane_iota(rows):
    return lax.broadcasted_iota(jnp.int32, (rows, N128), N1)


def store_flat(gbuf, vbuf, seg, row, base, back):
    cols = SHAPE[seg][N1]
    n = cols // N128
    step = N2 * n + N1
    low = lane_iota(RB // N2) < N64
    even = [vbuf[t, pl.ds(N0, RB // N2, stride=N2), :] for t in range(n + N1)]
    odd = [pltpu.roll(vbuf[t, pl.ds(N1, RB // N2, stride=N2), :], N64, N1) for t in range(n + N1)]
    start = base + lax.div(row, N2) * step
    for t in range(step):
        if t < n:
            v = even[t]
        elif t == n:
            v = jnp.where(low, even[n], odd[N0])
        else:
            v = jnp.where(low, odd[t - n - N1], odd[t - n])
        gbuf[pl.ds(start + t, RB // N2, stride=step), :] = pltpu.roll(v, back, N1)


def load_flat(pbuf, vbuf, seg, row, base, edge):
    cols = SHAPE[seg][N1]

    def take(at, rows, step):
        return jnp.where(lane_iota(rows) < edge, pbuf[pl.ds(at, rows, stride=step), :], pbuf[pl.ds(at + N1, rows, stride=step), :])
    if cols == FFN:
        for t in range(N20):
            vbuf[t] = take(base + row * N20 + t, RB, N20)
        return
    n = cols // N128
    step = N2 * n + N1
    low = lane_iota(RB // N2) < N64
    start = base + lax.div(row, N2) * step
    flat = [take(start + t, RB // N2, step) for t in range(step)]
    rolled = [pltpu.roll(v, N64, N1) for v in flat[n:]]
    for t in range(n + N1):
        vbuf[t, pl.ds(N0, RB // N2, stride=N2), :] = flat[t]
        v = rolled[t] if t == n else jnp.where(low, rolled[t], rolled[t + N1])
        vbuf[t, pl.ds(N1, RB // N2, stride=N2), :] = v


def seg_base(seg, core):
    if seg == "A":
        return core * 2400
    if seg == "B":
        return (N1 - core) * 7200
    return N0


def flat_shift(me):
    return N240 * jnp.where(me < N2, N4 - me, N8 - me)


def grad_window(me):
    offset = 2048 - flat_shift(me)
    shift = lax.rem(offset, N128)
    return lax.div(offset, N128), shift, lax.rem(N128 - shift, N128)


def late_kernel(gq, gk, gv, go, gflat, squares, oa, ob, ra, rb, ca, cb, vbuf,
                own_sem, pair_s, pair_r, hop_s, hop_r):
    me, core, chip = place()
    own, pair, box = dict(A=oa, B=ob), dict(A=ra, B=rb), dict(A=ca, B=cb)
    partner = peer(me, N1)
    _, _, back = grad_window(me)

    def source(seg, cc):
        return ((gq, go) if seg == "A" else (gk, gv))[cc]

    def own_copy(seg, cc):
        return pltpu.make_async_copy(source(seg, cc), own[seg], own_sem.at[SEG_ID[seg]])

    def pair_copy(seg, cc, half):
        i = N2 * SEG_ID[seg] + half
        at = pl.ds(half * HR, HR)
        return remote(source(seg, N1 - cc).at[at], pair[seg].at[at], pair_s.at[i], pair_r.at[i], partner)

    for cc in (N0, N1):
        @pl.when(core == cc)
        def _(cc=cc):
            own_copy("A", cc).start()
            own_copy("B", cc).start()
    greet(me)
    for cc in (N0, N1):
        @pl.when(core == cc)
        def _(cc=cc):
            for half in (N0, N1):
                for seg in "AB":
                    pair_copy(seg, cc, half).start()
    for seg in "AB":
        own_copy(seg, N0).wait()

    def ready(half):
        for seg in "AB":
            pair_copy(seg, N0, half).wait_recv()

    def add(seg, half, ch, with_hop):
        def body(i, carry):
            row = pl.multiple_of(half * HR + ch * CH + i * RB, RB)
            at = pl.ds(row, RB)
            v = own[seg][at, :].astype(F32) + pair[seg][at, :].astype(F32)
            own[seg][at, :] = v.astype(BF16)
            if with_hop:
                w = own[seg][at, :].astype(F32) + box[seg][at, :].astype(F32)
                own[seg][at, :] = w.astype(BF16)
            return carry
        lax.fori_loop(N0, CH // RB, body, N0)

    def hop_copy(seg, half, ch, to):
        i = N4 * ch + N2 * half + SEG_ID[seg]
        at = pl.ds(half * HR + ch * CH, CH)
        return remote(own[seg].at[at], box[seg].at[at], hop_s.at[i], hop_r.at[i], to)

    squares[...] = jnp.zeros((N8, N128), F32)
    paths = ((N2, N3, N1, N0), (N1, N3, N2, N0))
    for k in range(N4):
        @pl.when(chip == k)
        def _(k=k):
            sends = []
            if k == N0:
                ready(N0)
                ready(N1)
                total = jnp.zeros((N8, N128), F32)
                for ch in range(HR // CH):
                    for half in (N0, N1):
                        for seg in "AB":
                            hop_copy(seg, half, ch, partner).wait_recv()
                            base = seg_base(seg, core)
                            cols = SHAPE[seg][N1]

                            def body(i, acc, seg=seg, base=base, cols=cols, first=half * HR + ch * CH):
                                row = pl.multiple_of(first + i * RB, RB)
                                at = pl.ds(row, RB)
                                v = own[seg][at, :].astype(F32) + pair[seg][at, :].astype(F32) + box[seg][at, :].astype(F32)
                                sq = v * v
                                for t in range(cols // N128):
                                    part = sq[:, t * N128:(t + N1) * N128]
                                    acc = acc + part[:N8] + part[N8:]
                                    vbuf[t] = v[:, t * N128:(t + N1) * N128]
                                part = sq[:N8, cols - N64:] + sq[N8:, cols - N64:]
                                vbuf[cols // N128, :, :N64] = v[:, cols - N64:]
                                store_flat(gflat, vbuf, seg, row, base, back)
                                return acc + jnp.concatenate([part, jnp.zeros((N8, N64), F32)], axis=N1)
                            total = lax.fori_loop(N0, CH // RB, body, total)
                squares[...] = total
            else:
                spots = [paths[half].index(k) for half in (N0, N1)]
                halves = sorted((N0, N1), key=lambda half: spots[half])
                starts = [half for half in halves if spots[half] == N0]
                rest = [half for half in halves if spots[half] != N0]
                for group in (starts, rest):
                    for half in group:
                        ready(half)
                    for ch in range(HR // CH):
                        for half in group:
                            nxt = paths[half][spots[half] + N1]
                            to = N2 * nxt + core
                            for seg in "AB":
                                if group is rest:
                                    hop_copy(seg, half, ch, to).wait_recv()
                                add(seg, half, ch, group is rest)
                                c = hop_copy(seg, half, ch, to)
                                c.start()
                                sends.append(c)
            for c in sends:
                c.wait_send()
            for half in (N0, N1):
                for seg in "AB":
                    pair_copy(seg, N0, half).wait_send()


def late_scatter(grads):
    any_spec = pl.BlockSpec(memory_space=pl.ANY)
    vm = pl.BlockSpec(memory_space=pltpu.VMEM)
    dma = pltpu.SemaphoreType.DMA
    bufs = [pltpu.VMEM(SHAPE[s], BF16) for s in "AB"]
    return pl.pallas_call(
        late_kernel, in_specs=[any_spec] * N4, out_specs=[vm] * N2,
        out_shape=[jax.ShapeDtypeStruct((FLAT, N128), F32), jax.ShapeDtypeStruct((N8, N128), F32)],
        scratch_shapes=bufs * N3 + [pltpu.VMEM((N20, RB, N128), F32), dma((N2,)), dma((N4,)), dma((N4,)), dma((N20,)), dma((N20,))],
        compiler_params=pltpu.CompilerParams(collective_id=N1, has_side_effects=True, vmem_limit_bytes=N40 << N20),
        cost_estimate=pl.CostEstimate(flops=N10 ** N8, bytes_accessed=N10 ** N7, transcendentals=N0),
        name="late_scatter")(*grads)


BLK = 8192


def update_kernel(own_hbm, pair_hbm, x2, x3, y3, y2, flat_hbm, squares_in, gains, master, mean, var,
                  oa, ob, og, ou, od, heads_out, norm_out, master_out, mean_out, var_out,
                  ob_own, ob_pair, ob_x, ob_y, gbuf, vbuf, m32, tbuf, msg, gbox, mbox, p1, m1, v1,
                  pbuf, sa, sb, sg, sd, box, ends,
                  in_sem, state_sem, gain_s, gain_r, msg_s, msg_r, keep_sem, head_s, head_r, out_s, out_r):
    me, core, chip = place()
    partner = peer(me, N1)
    side = (peer(me, N2), peer(me, N4))
    shard = jnp.maximum(chip - N1, N0)
    skip, shift, back = grad_window(me)
    flat_in = pltpu.make_async_copy(flat_hbm, gbuf.at[pl.ds(N16, FLAT)], in_sem.at[N0])
    part_in = [pltpu.make_async_copy(own_hbm.at[shard], ob_own, in_sem.at[N1]),
               pltpu.make_async_copy(pair_hbm.at[shard], ob_pair, in_sem.at[N2]),
               pltpu.make_async_copy(x2.at[N1], ob_x.at[pl.ds(N0, HR)], in_sem.at[N3]),
               pltpu.make_async_copy(x3, ob_x.at[pl.ds(HR, HR)], in_sem.at[N4]),
               pltpu.make_async_copy(y3, ob_y.at[pl.ds(N0, HR)], in_sem.at[N5]),
               pltpu.make_async_copy(y2.at[N1], ob_y.at[pl.ds(HR, HR)], in_sem.at[N6])]

    @pl.when(chip == N0)
    def _():
        flat_in.start()

    @pl.when(chip != N0)
    def _():
        for c in part_in:
            c.start()
    state_in = [pltpu.make_async_copy(src, dst, state_sem.at[i])
                for i, (src, dst) in enumerate(((master, p1), (mean, m1), (var, v1)))]
    for c in state_in:
        c.start()
    greet(me)
    gain_copies = [remote(gains, gbox.at[me], gain_s.at[mask], gain_r.at[mask], peer(me, mask)) for mask in range(N1, N8)]
    for c in gain_copies:
        c.start()
    gbox[me] = gains[...]

    def summed(at, cols):
        return (ob_own[at, cols].astype(F32) + ob_pair[at, cols].astype(F32)) + (ob_x[at, cols].astype(F32) + ob_y[at, cols].astype(F32))

    @pl.when(chip == N0)
    def _():
        flat_in.wait()
        msg[N16:N24, :] = squares_in[...]

    @pl.when(chip != N0)
    def _():
        for c in part_in:
            c.wait()

    @pl.when(lax.rem(chip, N3) != N0)
    def _():
        def body(i, acc):
            row = pl.multiple_of(i * RB, RB)
            for half in (N0, N1):
                v = summed(pl.ds(pl.multiple_of(half * HR + row, RB), RB), slice(None))
                sq = v * v
                for t in range(HC // N128):
                    part = sq[:, t * N128:(t + N1) * N128]
                    acc = acc + part[:N8] + part[N8:]
                    gbuf[pl.ds(N16 + row * N20 + half * N10 + t, RB, stride=N20), :] = pltpu.roll(v[:, t * N128:(t + N1) * N128], back, N1)
            return acc
        msg[N16:N24, :] = lax.fori_loop(N0, HR // RB, body, jnp.zeros((N8, N128), F32))

    @pl.when(chip == N3)
    def _():
        def turn(t, acc):
            cols = pl.ds(pl.multiple_of(t * N128, N128), N128)
            for r in range(DIM // N128 + N1):
                n = min(N128, DIM - r * N128)
                v = summed(pl.ds(r * N128, n), cols)
                sq = v * v
                for u in range(n // N8):
                    acc = acc + sq[u * N8:(u + N1) * N8]
                m32[cols, r * N128:r * N128 + n] = v.T
            return acc
        msg[N16:N24, :] = lax.fori_loop(N0, HC // N128, turn, jnp.zeros((N8, N128), F32))

        def body(i, carry):
            row = pl.multiple_of(i * RB, RB)
            for t in range(N8):
                vbuf[t] = m32[pl.ds(row, RB), t * N128:(t + N1) * N128]
            store_flat(gbuf, vbuf, "D", row, N16, back)
            return carry
        lax.fori_loop(N0, HC // RB, body, N0)

    msg[N0:N16, :] = pltpu.roll(gbuf[FLAT:FLAT + N16, :], shift, N1)
    gbuf[FLAT + N16:FLAT + N32, :] = jnp.zeros((N16, N128), F32)
    msg_copies = []
    for mask in range(N1, N8):
        c = remote(msg, mbox.at[me], msg_s.at[mask], msg_r.at[mask], peer(me, mask))
        c.start()
        msg_copies.append(c)
    mbox[me] = msg[...]
    for c in gain_copies:
        c.wait()
    for c in msg_copies:
        c.wait()
    gain_sum = jnp.zeros((N16, N128), F32)
    squares = jnp.zeros((N8, N128), F32)
    for i in range(N8):
        gain_sum = gain_sum + gbox[i]
        squares = squares + mbox[i, N16:N24, :]
    squares = squares + gain_sum[:N8] * gain_sum[:N8] + gain_sum[N8:] * gain_sum[N8:]
    norm = jnp.sqrt(jnp.sum(squares, keepdims=True)) * 0.125
    norm_out[...] = jnp.broadcast_to(norm, (N8, N128))

    tail = mbox[lax.rem(me + N7, N8), N0:N16, :]
    gbuf[N0:N16, :] = tail
    low = lane_iota(N8) < N64

    def put_gain(g):
        r = pltpu.roll(g, N64, N1)
        gbuf[N8:N16, :] = jnp.where(low, pltpu.roll(r, N1, N0), r)

    @pl.when(me == N0)
    def _():
        put_gain(gain_sum[:N8])

    @pl.when(me == N2)
    def _():
        put_gain(gain_sum[N8:])
        tbuf[N0:N16, :] = pltpu.roll(tail, N64, N1)
        gbuf[N0:N8, :] = jnp.where(low, tbuf[N7:N15, :], tbuf[N8:N16, :])
        gbuf[N8:N9, :] = jnp.where(low[:N1], tbuf[N15:N16, :], gbuf[N8:N9, :])

    gbuf[N0:N16, :] = pltpu.roll(gbuf[N0:N16, :], back, N1)
    clip = jnp.minimum(F1_0, F1_0 / (norm + 1e-6)) * 0.125
    d = flat_shift(me)
    p_skip = lax.div(d, N128)
    p_back = lax.rem(N128 - lax.rem(d, N128), N128)
    gain_lo = jnp.where(me == N2, N480, N0)
    gain_hi = jnp.where(me == N0, DIM, jnp.where(me == N2, N480 + DIM, N0))
    for c in state_in:
        c.wait()

    def step(first, rows, p, m, v):
        low_lanes = lane_iota(rows) < N128 - shift
        a = gbuf[pl.ds(first + skip, rows), :]
        b = gbuf[pl.ds(first + skip + N1, rows), :]
        g = jnp.where(low_lanes, a, b) * clip
        m = BETA_ONE * m + (F1_0 - BETA_ONE) * g
        v = BETA_TWO * v + (F1_0 - BETA_TWO) * g * g
        m_hat = m * (F1_0 / (F1_0 - BETA_ONE ** STEP_COUNT))
        v_hat = v * (F1_0 / (F1_0 - BETA_TWO ** STEP_COUNT))
        at = (first + lax.broadcasted_iota(jnp.int32, (rows, N128), N0)) * N128 + lane_iota(rows)
        decays = jnp.where((at >= gain_lo) & (at < gain_hi), 0.0, WEIGHT_DECAY)
        return p - LEARN_RATE * (m_hat / (jnp.sqrt(v_hat) + ADAM_EPS) + decays * p), m, v

    def block(i, carry):
        at = pl.ds(pl.multiple_of(i * BLK, BLK), BLK)
        first = pl.multiple_of(i * N64, N64)
        p, m, v = step(first, N64, *[r[at].reshape(N64, N128) for r in (p1, m1, v1)])
        for r, w in ((p1, p), (m1, m), (v1, v)):
            r[at] = w.reshape(BLK)
        pbuf[pl.ds(first, N64), :] = pltpu.roll(p, p_back, N1)
        return p
    tbuf[...] = block(N0, jnp.zeros((N64, N128), F32))[:N16]
    head_copies = []
    for mask in range(N1, N8):
        c = remote(tbuf, box.at[me], head_s.at[mask], head_r.at[mask], peer(me, mask))
        c.start()
        head_copies.append(c)
    box[me] = tbuf[...]
    lax.fori_loop(N1, FLAT // N64, block, jnp.zeros((N64, N128), F32))
    last = pl.ds(FLAT * N128, N240)
    p, m, v = step(FLAT, N8, *[jnp.concatenate([r[last], jnp.zeros((784,), F32)]).reshape(N8, N128) for r in (p1, m1, v1)])
    for r, w in ((p1, p), (m1, m), (v1, v)):
        r[last] = w.reshape(N1024)[:N240]
    ends[N0:N8, :] = p
    state_out = [pltpu.make_async_copy(src, dst, state_sem.at[i])
                 for i, (src, dst) in enumerate(((p1, master_out), (m1, mean_out), (v1, var_out)))]
    for c in state_out:
        c.start()
    for c in head_copies:
        c.wait()
    heads_out[N0] = box[N0]
    heads_out[N1] = box[N2]
    nxt = pltpu.roll(box[lax.rem(me + N1, N8)], N112, N1)
    keep = lane_iota(N1) < N112
    ends[N1:N2, :] = jnp.where(keep, ends[N1:N2, :], nxt[N0:N1])
    ends[N2:17, :] = jnp.where(lane_iota(N15) < N112, nxt[N0:N15], nxt[N1:N16])
    pbuf[FLAT:FLAT + N24, :] = pltpu.roll(ends[...], p_back, N1)
    edge = N128 - lax.rem(d, N128)
    stage = dict(A=sa, B=sb, G=sg, U=sg, D=sd)

    def matrix(seg, flip):
        rows, cols = SHAPE[seg]
        base = seg_base(seg, core)

        def body(i, carry):
            row = pl.multiple_of(i * RB, RB)
            load_flat(pbuf, vbuf, seg, row, base + p_skip, edge)
            for t in range(pl.cdiv(cols, N128)):
                if flip:
                    m32[pl.ds(row, RB), t * N128:(t + N1) * N128] = vbuf[t]
                else:
                    stage[seg][pl.ds(row, RB), t * N128:(t + N1) * N128] = vbuf[t].astype(BF16)
            return carry
        lax.fori_loop(N0, rows // RB, body, N0)
        if flip:
            for r in range(pl.cdiv(rows, N128)):
                for t in range(pl.cdiv(cols, N128)):
                    blk = m32[r * N128:(r + N1) * N128, t * N128:(t + N1) * N128]
                    stage[seg][t * N128:(t + N1) * N128, r * N128:(r + N1) * N128] = blk.T.astype(BF16)

    def sizes(seg):
        return {"A": N960, "B": N320, "G": N480, "U": N480, "D": N960}[seg]

    def staged(seg, part):
        n = sizes(seg) // N2
        return stage[seg].at[pl.ds(part * n, n)]

    def target(seg, part):
        n = sizes(seg) // N2
        if seg == "A":
            return oa.at[core, pl.ds(part * n, n)]
        if seg == "B":
            return ob.at[core, pl.ds(part * n, n)]
        if seg == "D":
            return od.at[pl.ds(part * n, n), pl.ds(pl.multiple_of(core * N1280, N128), N1280)]
        ref = og if seg == "G" else ou
        return ref.at[pl.ds(core * N480 + part * n, n)]

    def slot(origin, part, piece):
        return origin * N4 + part * N2 + piece

    for k in range(N4):
        x, y, z = k ^ N1, k ^ N2, k ^ N3

        @pl.when(chip == k)
        def _(k=k, x=x, y=y, z=z):
            sends, keeps = [], []

            def go(src, dst, send, recv_slot, to):
                c = remote(src, dst, out_s.at[send], out_r.at[recv_slot], to)
                c.start()
                sends.append(c)

            def arrived(ref, i):
                remote(ref, ref, out_s.at[N0], out_r.at[i], partner).wait_recv()

            for seg in SEGS[k]:
                if seg == "A":
                    @pl.when(core == N0)
                    def _():
                        matrix("A", True)

                    @pl.when(core == N1)
                    def _():
                        matrix("A", False)
                else:
                    matrix(seg, seg in "BD")
            n_send = [N0]

            def nid():
                n_send[N0] += N1
                return n_send[N0] - N1

            for order in (N0, N1):
                for which in (N0, N1):
                    part = which if order == N0 else N1 - which
                    for piece, seg in enumerate(SEGS[k]):
                        go(staged(seg, part), target(seg, part), nid(), slot(N1 + which, part, piece), side[which])
            for part in (N0, N1):
                for piece, seg in enumerate(SEGS[k]):
                    go(staged(seg, part), target(seg, part), nid(), N16 + slot(N0, part, piece), partner)
                    c = pltpu.make_async_copy(staged(seg, part), target(seg, part), keep_sem.at[N2 * part + piece])
                    c.start()
                    keeps.append(c)
            for which, s in ((N0, x), (N1, y)):
                for piece, seg in enumerate(SEGS[s]):
                    ref = target(seg, which)
                    arrived(ref, slot(N1 + which, which, piece))
                    go(ref, ref, nid(), slot(N3, which, piece), side[N1 - which])
                    go(ref, ref, nid(), N16 + slot(N1 + which, which, piece), partner)
            for which, s in ((N0, x), (N1, y)):
                for piece, seg in enumerate(SEGS[s]):
                    ref = target(seg, N1 - which)
                    arrived(ref, slot(N1 + which, N1 - which, piece))
                    go(ref, ref, nid(), N16 + slot(N1 + which, N1 - which, piece), partner)
            for part in (N0, N1):
                for piece, seg in enumerate(SEGS[z]):
                    ref = target(seg, part)
                    arrived(ref, slot(N3, part, piece))
                    go(ref, ref, nid(), N16 + slot(N3, part, piece), partner)
            for origin, s in ((N0, k), (N1, x), (N2, y), (N3, z)):
                for part in (N0, N1):
                    for piece, seg in enumerate(SEGS[s]):
                        arrived(target(seg, part), N16 + slot(origin, part, piece))
            for c in sends:
                c.wait_send()
            for c in keeps:
                c.wait()
    for c in state_out:
        c.wait()


def update(own, pair, hops, flat, squares, gains, master, mean, var):
    any_spec = pl.BlockSpec(memory_space=pl.ANY)
    vm = pl.BlockSpec(memory_space=pltpu.VMEM)
    dma = pltpu.SemaphoreType.DMA
    shapes = [(N2, DIM, N1024), (N2, N320, N1024), (DIM, FFN), (DIM, FFN), (DIM, FFN)]
    state = jax.ShapeDtypeStruct(master.shape, F32)
    return pl.pallas_call(
        update_kernel,
        in_specs=[any_spec] * N7 + [vm] * N2 + [any_spec] * N3, out_specs=[any_spec] * N5 + [vm] * N2 + [any_spec] * N3,
        out_shape=[jax.ShapeDtypeStruct(s, BF16) for s in shapes] + [jax.ShapeDtypeStruct((N2, N16, N128), F32),
                   jax.ShapeDtypeStruct((N8, N128), F32), state, state, state],
        scratch_shapes=[pltpu.VMEM((DIM, HC), BF16)] * N4
                       + [pltpu.VMEM((FLAT + N32, N128), F32), pltpu.VMEM((N20, RB, N128), F32), pltpu.VMEM((HC, N1024), F32),
                          pltpu.VMEM((N16, N128), F32), pltpu.VMEM((N24, N128), F32), pltpu.VMEM((N8, N16, N128), F32),
                          pltpu.VMEM((N8, N24, N128), F32)]
                       + [pltpu.VMEM(master.shape, F32)] * N3
                       + [pltpu.VMEM((LOCAL + N16, N128), F32), pltpu.VMEM((N1024, N1024), BF16), pltpu.VMEM((384, N1024), BF16),
                          pltpu.VMEM((HR, FFN), BF16), pltpu.VMEM((N1024, HC), BF16), pltpu.VMEM((N8, N16, N128), F32), pltpu.VMEM((N24, N128), F32)]
                       + [dma((N7,)), dma((N3,)), dma((N8,)), dma((N8,)), dma((N8,)), dma((N8,)), dma((N4,)), dma((N8,)), dma((N8,)),
                          dma((N40,)), dma((N32,))],
        compiler_params=pltpu.CompilerParams(collective_id=N2, has_side_effects=True, vmem_limit_bytes=67043328),
        name="update")(own, pair, *hops, flat, squares, gains, master, mean, var)


def solution(mesh):
    def per_device(x, dy, pos, attn_gain, w_query, w_key, w_value, w_out, mlp_gain, w_gate, w_up, w_down, master, mean, var):
        def cd(w, n):
            return jnp.transpose(w, (N1, N2, N0)).reshape(n, DIM)

        def back(w, n):
            return jnp.transpose(w.reshape(n, HD, DIM), (N2, N0, N1))
        d_x, attn_grads, (own, pair, hops), (g_ag, g_mg) = local_grads(
            x[N0].T, dy[N0].T, pos[N0], attn_gain, cd(w_query, DIM), cd(w_key, N320), cd(w_value, N320),
            w_out.reshape(DIM, DIM), mlp_gain, w_gate, w_up, w_down.T)
        gains = jnp.stack([jnp.pad(g.astype(F32), (N0, N64)) for g in (g_ag, g_mg)]).reshape(N16, N128)
        flat, squares = late_scatter(attn_grads)
        oa, ob, og, ou, od, heads, norm, new_master, new_mean, new_var = update(
            own, pair, hops, flat, squares, gains, master, mean, var)
        grad_norm = norm[N0, N0]
        heads = heads.reshape(N2, 2048).astype(BF16)
        new = (heads[N0, :DIM], back(oa[N0, :, :DIM], HEADS), back(ob[N0, :, :DIM], KVH), back(ob[N1, :, :DIM], KVH),
               oa[N1, :, :DIM].reshape(HEADS, HD, DIM), heads[N1, N480:N480 + DIM], og, ou, od.T)
        return (d_x.T[None],) + new + (new_master, new_mean, new_var, grad_norm)
    in_specs = (P('dp'),) * N3 + (P(),) * N9 + (P('dp'),) * N3
    out_specs = (P('dp'),) + (P(),) * N9 + (P('dp'),) * N3 + (P(),)
    return jax.shard_map(per_device, mesh=mesh, in_specs=in_specs, out_specs=out_specs, check_vma=False)
```
